32 devices in a mesh: ep: 4 (over x, core), fsdp: 8 (over z, y).
Axes of the slice: x: 2, y: 2, z: 4, core: 2. Of those that a mesh axis runs over, the one named last changes fastest.
Arguments:
- master_gate: float32 [128, 2048, 768], P('ep', 'fsdp'), may hold values from -0.1875 to 0.1875
- master_up: float32 [128, 2048, 768], P('ep', 'fsdp'), may hold values from -0.1875 to 0.1875
- router_weight: float32 [2048, 128], P('fsdp', 'ep'), may hold values from -0.125 to 0.125
- router_gain: float32 [2048], P('fsdp'), may hold values from 0.25 to 1.75
Outputs:
- final_gate: bfloat16 [128, 2048, 768], P(('ep', 'fsdp'))
- final_up: bfloat16 [128, 2048, 768], P(('ep', 'fsdp'))
- scale_gate: float32 [128, 768], P(('ep', 'fsdp'))
- scale_up: float32 [128, 768], P(('ep', 'fsdp'))
- serve_router: bfloat16 [2048, 128], replicated
The draws below stay inside these ranges and needn't reach their ends.
All inputs are finite; a program needn't handle non-finite values.
Results may differ from the reference program's by a relative error of at most 0.001.
Values may be sent and summed in bfloat16 or wider, within the bound.
A program may use at most 192 MiB of HBM per device.

```python
import jax
import jax.numpy as jnp
from jax import lax

EXPERTS = 128
D_MODEL = 2048
D_EXPERT = 768


def with_spikes(drawn, own_key, source, target, blocks, factor):
    owner, partner = [(jnp.arange(drawn.shape[axis_at]) // (drawn.shape[axis_at] // blocks)).reshape([-1 if axis == axis_at else 1 for axis in range(drawn.ndim)]) for axis_at in (source, target)]
    chosen = jax.random.permutation(own_key, blocks)[partner]
    strong = (owner == chosen) | (owner == (partner + blocks // 2) % blocks)
    return jnp.where(strong, factor * drawn, drawn)


def level_of(stream_key, dims, pieces, least, high):
    loudness = 1.0
    for dim, parts in pieces:
        heights = jax.random.uniform(jax.random.fold_in(jax.random.fold_in(stream_key, 6), dim), (parts,), jnp.float32, least / len(pieces), high / len(pieces))
        loudness = loudness * jnp.repeat(jnp.exp(heights), dims[dim] // parts).reshape((-1,) + (1,) * (len(dims) - 1 - dim))
    return loudness


def noise(rng, shape, scale, limit, pieces=(), kind=jnp.bfloat16):
    result = scale * jax.random.normal(rng, shape, jnp.float32)
    if pieces:
        result = result * level_of(rng, shape, pieces, -0.22, 0.18)
    return jnp.clip(result, -limit, limit).astype(kind)


def gaussian_with(stream_key, extent, spread, most, cuts, heavy, kind=jnp.bfloat16):
    result = spread * jax.random.normal(stream_key, extent, jnp.float32)
    if cuts:
        result = result * level_of(stream_key, extent, cuts, -0.22, 0.18)
    return jnp.clip(with_spikes(result, jax.random.fold_in(stream_key, 3), *heavy), -most, most).astype(kind)


def setup_inputs(seed: int = 0) -> dict:
    streams_of = jax.random.split(jax.random.key(seed), 5)
    return {
        "master_gate": gaussian_with(streams_of[0], (EXPERTS, D_MODEL, D_EXPERT), D_MODEL ** -0.5, 0.1875, ((0, 4), (1, 8)), (1, 2, 8, 2.0), jnp.float32),
        "master_up": gaussian_with(streams_of[1], (EXPERTS, D_MODEL, D_EXPERT), D_MODEL ** -0.5, 0.1875, ((0, 4), (1, 8)), (1, 2, 8, 2.0), jnp.float32),
        "router_weight": noise(streams_of[2], (D_MODEL, EXPERTS), D_MODEL ** -0.5, 0.125, ((0, 8), (1, 4)), jnp.float32),
        "router_gain": jnp.clip(1.0 + 0.15 * jax.random.normal(streams_of[3], (D_MODEL,), jnp.float32), 0.25, 1.75),
    }


def reference(master_gate, master_up, router_weight, router_gain):
    scale_gate = jnp.sqrt(lax.optimization_barrier(jnp.sum(master_gate * master_gate, axis=1)))
    final_gate = (master_gate / jnp.expand_dims(scale_gate, 1)).astype(jnp.bfloat16)
    scale_up = jnp.sqrt(lax.optimization_barrier(jnp.sum(master_up * master_up, axis=1)))
    final_up = (master_up / jnp.expand_dims(scale_up, 1)).astype(jnp.bfloat16)
    serve_router = (router_weight * router_gain[:, None]).astype(jnp.bfloat16)
    return (final_gate, final_up, scale_gate, scale_up, serve_router)
```

```python
import functools

import jax
import jax.numpy as jnp
from jax import lax
from jax.experimental import pallas as pl
from jax.experimental.pallas import tpu as pltpu
from jax.sharding import PartitionSpec as P

MESH = pl.DeviceIdType.MESH
RING = 2
SLOTS = 3
LANES = 128
UNITS = 8
GROUPS = ((0, 1), (1, 2), (3, 2), (5, 1), (6, 2))


def kernel(
    groups, members, local, rows,
    gate, up, weight, gain,
    final_gate, final_up, scale_gate, scale_up, serve,
    held, narrow, raw, stage,
    first, first_in, first_scales,
    late, near_in, far_in, total_far, far_total, scales,
    weight_in, gain_in, part_router, router,
    load_sem, send_sem, recv_sem, group_send, group_recv,
    first_send, first_recv, fscale_send, fscale_recv,
    raw_send, raw_recv, near_send, near_recv, cross_send, cross_recv,
    scale_send, scale_recv, relay_send, relay_recv,
    row_send, row_recv, col_send, col_recv, in_sem,
):
    group, me = lax.axis_index("ep"), lax.axis_index("fsdp")
    steps = 2 * local
    half = members // 2
    side, place_in_half = me // half, lax.rem(me, half)
    unit = rows // UNITS

    def peer(j):
        return lax.rem(me + j, members)

    def back(j):
        return lax.rem(me + members - j, members)

    def near_peer(n):
        return side * half + lax.rem(place_in_half + n, half)

    def far_peer(n):
        return (1 - side) * half + lax.rem(place_in_half + n, half)

    def offset(device):
        return lax.rem(device + members - me, members)

    def is_far(device):
        return device // half != side

    def group_peer(j):
        return lax.rem(group + j, groups)

    def remote(source, target, send, recv, member):
        return pltpu.make_async_remote_copy(
            src_ref=source, dst_ref=target, send_sem=send, recv_sem=recv,
            device_id=(group, member), device_id_type=MESH,
        )

    def source(step):
        return (gate, up)[step // local], (final_gate, final_up)[step // local], step % local

    order = [*range(1, steps), *range(1, steps)]

    def load(step, slot, j):
        master, _, index = source(step)
        return pltpu.make_async_copy(
            master.at[peer(j) * local + index], held.at[slot, j], load_sem.at[slot, j]
        )

    def start_load(step, slot):
        @pl.loop(0, members)
        def _(j):
            load(step, slot, j).start()

    def start_place(place):
        if place < len(order):
            start_load(order[place], 1 + place % RING)

    def rows_of(member):
        return pl.ds(pl.multiple_of(member * rows, rows), rows)

    def data_copy(step, j):
        _, final, index = source(step)
        return remote(
            narrow.at[step % SLOTS, j], final.at[index, rows_of(me), :],
            send_sem.at[step, j], recv_sem.at[step, j], peer(j),
        )

    def group_copy(g, j, far):
        begin, count = GROUPS[g]
        begin, count = begin * unit, count * unit
        there = pl.ds(pl.multiple_of(me * rows + begin, unit), count)
        columns = slice(LANES, None) if far else slice(None)
        return remote(
            narrow.at[0, j, begin : begin + count, columns], final_gate.at[0, there, columns],
            group_send.at[g, j], group_recv.at[g, j], peer(j),
        )

    def each_group_copy(g, sending, act):
        @pl.loop(1, members)
        def _(j):
            other = peer(j) if sending else back(j)

            @pl.when(is_far(other))
            def _():
                act(group_copy(g, j, True))

            @pl.when(jnp.logical_not(is_far(other)))
            def _():
                act(group_copy(g, j, False))

    def first_copy(j):
        return remote(first.at[j], first_in.at[j], first_send.at[j], first_recv.at[j], peer(j))

    def first_scale_copy(j):
        return remote(
            first_scales.at[0], first_scales.at[j], fscale_send.at[j], fscale_recv.at[j], peer(j)
        )

    def raw_copy(piece, n):
        count = rows // 2
        part = slice(piece * count, (piece + 1) * count)
        return remote(
            raw.at[n, part, :], stage.at[n, part, :],
            raw_send.at[piece, n], raw_recv.at[piece, n], far_peer(n),
        )

    def near_copy(n, far):
        owner = far_peer(n) if far else near_peer(n)
        return remote(
            late.at[offset(owner)], (far_in if far else near_in).at[n],
            near_send.at[int(far), n], near_recv.at[int(far), n], near_peer(n),
        )

    def cross_copy():
        return remote(total_far, far_total, cross_send.at[0], cross_recv.at[0], far_peer(0))

    def scale_copy(n):
        return remote(scales.at[0], scales.at[n], scale_send.at[n], scale_recv.at[n], near_peer(n))

    def far_scale_copy():
        return remote(
            scales.at[0], scales.at[half], scale_send.at[0], scale_recv.at[0], far_peer(0)
        )

    def relay_scale_copy(n):
        return remote(
            scales.at[half], scales.at[half + n], relay_send.at[n], relay_recv.at[n], near_peer(n)
        )

    def scale_slot(device):
        n = lax.rem(place_in_half + half - lax.rem(device, half), half)
        return jnp.where(is_far(device), half, 0) + n

    width, depth = part_router.shape
    my_group_rows = pl.ds(pl.multiple_of(group * width, width), width)
    my_columns = pl.ds(pl.multiple_of(me * depth, depth), depth)
    near = [*range(1, half), half]

    def row_peer(j):
        return far_peer(0) if j == half else near_peer(j)

    def row_copy(j):
        return remote(
            part_router, router.at[my_group_rows, my_columns],
            row_send.at[j], row_recv.at[j], row_peer(j),
        )

    def relay_copy(j):
        other = pl.ds(pl.multiple_of(far_peer(0) * depth, depth), depth)
        block = router.at[my_group_rows, other]
        return remote(block, block, row_send.at[half + j], row_recv.at[half + j], near_peer(j))

    def col_copy(j):
        return pltpu.make_async_remote_copy(
            src_ref=router.at[my_group_rows, :], dst_ref=router.at[my_group_rows, :],
            send_sem=col_send.at[j], recv_sem=col_recv.at[j],
            device_id=(group_peer(j), me), device_id_type=MESH,
        )

    barrier = pltpu.get_barrier_semaphore()
    for j in range(1, members):
        pl.semaphore_signal(barrier, inc=1, device_id=(group, peer(j)), device_id_type=MESH)
    for j in range(1, groups):
        pl.semaphore_signal(barrier, inc=1, device_id=(group_peer(j), me), device_id_type=MESH)

    start_load(0, 0)
    for place in range(RING):
        start_place(place)
    weight_copy = pltpu.make_async_copy(weight, weight_in, in_sem.at[0])
    gain_copy = pltpu.make_async_copy(gain, gain_in, in_sem.at[1])
    weight_copy.start()
    gain_copy.start()

    def sums(step, slot):
        @pl.loop(0, members)
        def _(j):
            load(step, slot, j).wait()
            block = held[slot, j]
            value = jnp.sum(block * block, axis=0, keepdims=True)
            if step == 0:
                first[j] = value
            else:
                late[j, step - 1] = value

    def late_sums(begin, end):
        for step in range(begin, min(end, steps)):
            sums(step, 1 + (step - 1) % RING)
            start_place(step - 1 + RING)

    def finish(step, value):
        index = step % local
        (scale_gate, scale_up)[step // local][index : index + 1, :] = value

    def keep_own(step, slot, inverse):
        _, final, index = source(step)
        final[index, rows_of(me), :] = (held[slot, 0] * inverse).astype(jnp.bfloat16)

    sums(0, 0)

    pl.semaphore_wait(barrier, members + groups - 2)

    @pl.loop(1, members)
    def _(j):
        first_copy(j).start()

    @pl.loop(0, half)
    def _(n):
        raw[n] = held[0, offset(far_peer(n)), :, 0:LANES].astype(jnp.bfloat16)

    @pl.loop(0, half)
    def _(n):
        raw_copy(0, n).start()

    late_sums(1, 3)

    @pl.loop(1, members)
    def _(j):
        first_copy(j).wait_recv()

    value = first[0]
    for j in range(1, members):
        value = value + first_in[j]
    value = jnp.sqrt(value)
    first_scales[0] = value
    finish(0, value)

    @pl.loop(1, members)
    def _(j):
        first_scale_copy(j).start()

    @pl.loop(0, half)
    def _(n):
        raw_copy(1, n).start()

    late_sums(3, 6)

    @pl.loop(1, members)
    def _(j):
        first_scale_copy(j).wait_recv()

    @pl.loop(1, members)
    def _(j):
        inverse = 1.0 / first_scales[lax.rem(members - j, members)]
        narrow[0, j] = (held[0, j] * inverse).astype(jnp.bfloat16)

    def start_group(g):
        each_group_copy(g, True, lambda copy: copy.start())

    start_group(0)

    late_sums(6, steps)

    for n in range(1, half):
        for far in (True, False):
            near_copy(n, far).start()

    start_group(1)

    my_inverse = 1.0 / first_scales[0]
    keep_own(0, 0, my_inverse)

    weight_copy.wait()
    gain_copy.wait()
    part_router[...] = (weight_in[...] * gain_in[...]).astype(jnp.bfloat16)
    router[my_group_rows, my_columns] = part_router[...]

    @pl.loop(0, half)
    def _(n):
        for piece in range(2):
            raw_copy(piece, n).wait_recv()
        from_member = (1 - side) * half + lax.rem(place_in_half + half - n, half)
        block = stage[n].astype(jnp.float32) * my_inverse[:, 0:LANES]
        final_gate[0, rows_of(from_member), 0:LANES] = block.astype(jnp.bfloat16)

    for n in range(1, half):
        for far in (True, False):
            near_copy(n, far).wait_recv()
    gathered = late[half]
    for n in range(1, half):
        gathered = gathered + far_in[n]
    total_far[...] = gathered
    cross_copy().start()

    start_group(2)

    gathered = late[0]
    for n in range(1, half):
        gathered = gathered + near_in[n]
    cross_copy().wait_recv()
    scales[0] = jnp.sqrt(gathered + far_total[...])
    far_scale_copy().start()
    for n in range(1, half):
        scale_copy(n).start()

    start_group(3)

    for step in range(1, steps):
        finish(step, scales[0, step - 1])

    far_scale_copy().wait_recv()
    for n in range(1, half):
        relay_scale_copy(n).start()

    start_group(4)

    for j in near:
        row_copy(j).start()

    for n in range(1, half):
        scale_copy(n).wait_recv()
        relay_scale_copy(n).wait_recv()

    def wait_sent(step):
        if step == 0:
            for g in range(len(GROUPS)):
                each_group_copy(g, True, lambda copy: copy.wait_send())
        else:
            @pl.loop(1, members)
            def _(j):
                data_copy(step, j).wait_send()

    def scale_and_send(step, slot):
        if step >= SLOTS:
            wait_sent(step - SLOTS)

        @pl.loop(1, members)
        def _(j):
            load(step, slot, j).wait()
            inverse = 1.0 / scales[scale_slot(peer(j)), step - 1]
            narrow[step % SLOTS, j] = (held[slot, j] * inverse).astype(jnp.bfloat16)

        @pl.loop(1, members)
        def _(j):
            data_copy(step, j).start()

        load(step, slot, 0).wait()
        keep_own(step, slot, 1.0 / scales[0, step - 1])

    for step in range(1, steps):
        place = steps - 2 + step
        scale_and_send(step, 1 + place % RING)
        start_place(place + RING)
        if step == steps // 2:
            for j in near:
                row_copy(j).wait()
            for j in range(1, half):
                relay_copy(j).start()

    for j in range(1, half):
        relay_copy(j).wait()
    for j in range(1, groups):
        col_copy(j).start()

    @pl.loop(1, members)
    def _(j):
        first_copy(j).wait_send()
        first_scale_copy(j).wait_send()

    @pl.loop(0, half)
    def _(n):
        for piece in range(2):
            raw_copy(piece, n).wait_send()

    for n in range(1, half):
        for far in (True, False):
            near_copy(n, far).wait_send()
        scale_copy(n).wait_send()
        relay_scale_copy(n).wait_send()
    cross_copy().wait_send()
    far_scale_copy().wait_send()

    for j in range(1, groups):
        col_copy(j).wait()

    @pl.loop(0, router.shape[1] // LANES)
    def _(block):
        here = pl.ds(pl.multiple_of(block * LANES, LANES), LANES)
        serve[here, :] = router[:, here].astype(jnp.float32).T.astype(jnp.bfloat16)

    for step in range(steps):
        if step >= steps - SLOTS:
            wait_sent(step)
        if step == 0:
            for g in range(len(GROUPS)):
                each_group_copy(g, False, lambda copy: copy.wait_recv())
        else:
            @pl.loop(1, members)
            def _(j):
                data_copy(step, j).wait_recv()


def exchange(groups, members, master_gate, master_up, weight, gain):
    experts, rows, inner = master_gate.shape
    local = experts // members
    steps = 2 * local
    half = members // 2
    width, depth = weight.shape
    in_hbm = pl.BlockSpec(memory_space=pltpu.HBM)
    in_vmem = pl.BlockSpec(memory_space=pltpu.VMEM)
    final = pltpu.VMEM((local, members * rows, inner), jnp.bfloat16)
    scale = pltpu.VMEM((local, inner), jnp.float32)
    dma = pltpu.SemaphoreType.DMA

    def sums(*shape):
        return pltpu.VMEM((*shape, 1, inner), jnp.float32)

    late = steps - 1
    return pl.pallas_call(
        functools.partial(kernel, groups, members, local, rows),
        out_shape=(
            final, final, scale, scale,
            pltpu.VMEM((members * depth, groups * width), jnp.bfloat16),
        ),
        in_specs=[in_hbm] * 4,
        out_specs=(in_vmem,) * 5,
        scratch_shapes=[
            pltpu.VMEM((1 + RING, members, rows, inner), jnp.float32),
            pltpu.VMEM((SLOTS, members, rows, inner), jnp.bfloat16),
            pltpu.VMEM((half, rows, LANES), jnp.bfloat16),
            pltpu.VMEM((half, rows, LANES), jnp.bfloat16),
            sums(members), sums(members), sums(members),
            sums(members, late), sums(half, late), sums(half, late),
            sums(late), sums(late), sums(members, late),
            pltpu.VMEM((width, depth), jnp.float32),
            pltpu.VMEM((1, depth), jnp.float32),
            pltpu.VMEM((width, depth), jnp.bfloat16),
            pltpu.VMEM((groups * width, members * depth), jnp.bfloat16),
            dma((1 + RING, members)),
            dma((steps, members)), dma((steps, members)),
            dma((len(GROUPS), members)), dma((len(GROUPS), members)),
            dma((members,)), dma((members,)), dma((members,)), dma((members,)),
            dma((2, half)), dma((2, half)), dma((2, half)), dma((2, half)), dma((1,)), dma((1,)),
            dma((half,)), dma((half,)), dma((half,)), dma((half,)),
            dma((members,)), dma((members,)), dma((groups,)), dma((groups,)), dma((2,)),
        ],
        compiler_params=pltpu.CompilerParams(
            collective_id=0, has_side_effects=True, vmem_limit_bytes=35 * 1024 * 1024
        ),
    )(master_gate, master_up, weight, gain)


def store_kernel(*refs):
    count = (len(refs) - 1) // 2
    sem = refs[-1]
    copies = []
    for landed, stored in zip(refs[:count], refs[count:-1]):
        if len(landed.shape) == 3:
            pairs = [(landed.at[i], stored.at[i]) for i in range(landed.shape[0])]
        else:
            pairs = [(landed, stored)]
        for here, there in pairs:
            copies.append(pltpu.make_async_copy(here, there, sem.at[len(copies)]))
    for copy in copies:
        copy.start()
    for copy in copies:
        copy.wait()


def store(*landed):
    pieces = sum(array.shape[0] if array.ndim == 3 else 1 for array in landed)
    return pl.pallas_call(
        store_kernel,
        out_shape=tuple(jax.ShapeDtypeStruct(array.shape, array.dtype) for array in landed),
        in_specs=[pl.BlockSpec(memory_space=pltpu.VMEM)] * len(landed),
        out_specs=(pl.BlockSpec(memory_space=pl.ANY),) * len(landed),
        scratch_shapes=[pltpu.SemaphoreType.DMA((pieces,))],
        compiler_params=pltpu.CompilerParams(vmem_limit_bytes=2 * 1024 * 1024),
    )(*landed)


def solution(mesh):
    groups, members = mesh.shape["ep"], mesh.shape["fsdp"]

    def body(master_gate, master_up, router_weight, router_gain):
        landed = exchange(
            groups, members, master_gate, master_up, router_weight.T, router_gain[None, :]
        )
        return store(*landed)

    return jax.shard_map(
        body,
        mesh=mesh,
        in_specs=(P("ep", "fsdp", None), P("ep", "fsdp", None), P("fsdp", "ep"), P("fsdp")),
        out_specs=(
            P(("ep", "fsdp"), None, None),
            P(("ep", "fsdp"), None, None),
            P(("ep", "fsdp"), None),
            P(("ep", "fsdp"), None),
            P(),
        ),
        check_vma=False,
    )
```

```python
import functools

import jax
import jax.numpy as jnp
from jax import lax
from jax.experimental import pallas as pl
from jax.experimental.pallas import tpu as pltpu
from jax.sharding import PartitionSpec as P

MESH = pl.DeviceIdType.MESH
RING = 2
SLOTS = 3
LANES = 128
UNITS = 8
GROUPS = ((0, 1), (1, 2), (3, 2), (5, 1), (6, 2))
KEPT_UNITS = 6


def in_middle(member, members):
    return jnp.logical_and(member >= members // 4, member < members - members // 4)


def partner_of(member, members):
    return jnp.where(member < members // 2, member + members // 4, member - members // 4)


def kernel(
    groups, members, local, rows,
    gate, up, weight, gain,
    final_gate, final_up, scale_gate, scale_up, serve, kept,
    held, narrow, raw, stage,
    first, first_in, first_scales,
    late, near_in, far_in, total_far, far_total, scales,
    weight_in, gain_in, part_router, router,
    load_sem, send_sem, recv_sem, group_send, group_recv,
    first_send, first_recv, fscale_send, fscale_recv,
    raw_send, raw_recv, near_send, near_recv, cross_send, cross_recv,
    scale_send, scale_recv, relay_send, relay_recv,
    row_send, row_recv, col_send, col_recv, in_sem,
):
    group, me = lax.axis_index("ep"), lax.axis_index("fsdp")
    steps = 2 * local
    half = members // 2
    side, place_in_half = me // half, lax.rem(me, half)
    unit = rows // UNITS

    def peer(j):
        return lax.rem(me + j, members)

    def back(j):
        return lax.rem(me + members - j, members)

    def near_peer(n):
        return side * half + lax.rem(place_in_half + n, half)

    def far_peer(n):
        return (1 - side) * half + lax.rem(place_in_half + n, half)

    def offset(device):
        return lax.rem(device + members - me, members)

    def is_far(device):
        return device // half != side

    def group_peer(j):
        return lax.rem(group + j, groups)

    def remote(source, target, send, recv, member):
        return pltpu.make_async_remote_copy(
            src_ref=source, dst_ref=target, send_sem=send, recv_sem=recv,
            device_id=(group, member), device_id_type=MESH,
        )

    def source(step):
        return (gate, up)[step // local], (final_gate, final_up)[step // local], step % local

    order = [*range(1, steps), *range(1, steps)]

    def load(step, slot, j):
        master, _, index = source(step)
        return pltpu.make_async_copy(
            master.at[peer(j) * local + index], held.at[slot, j], load_sem.at[slot, j]
        )

    def start_load(step, slot):
        @pl.loop(0, members)
        def _(j):
            load(step, slot, j).start()

    def start_place(place):
        if place < len(order):
            start_load(order[place], 1 + place % RING)

    def rows_of(member):
        return pl.ds(pl.multiple_of(member * rows, rows), rows)

    def data_copy(step, j):
        _, final, index = source(step)
        return remote(
            narrow.at[step % SLOTS, j], final.at[index, rows_of(me), :],
            send_sem.at[step, j], recv_sem.at[step, j], peer(j),
        )

    kept_rows = KEPT_UNITS * unit
    partner = partner_of(me, members)

    def short_copy(j):
        step = steps - 1
        count = rows - kept_rows
        there = pl.ds(pl.multiple_of(me * rows, rows), count)
        return remote(
            narrow.at[step % SLOTS, j, 0:count], final_up.at[local - 1, there, :],
            send_sem.at[step, j], recv_sem.at[step, j], peer(j),
        )

    def each_data_copy(step, sending, act):
        @pl.loop(1, members)
        def _(j):
            if step < steps - 1:
                act(data_copy(step, j))
            else:
                other = peer(j) if sending else back(j)
                short = jnp.logical_and(in_middle(me, members), other == partner)

                @pl.when(jnp.logical_not(short))
                def _():
                    act(data_copy(step, j))

                if kept_rows < rows:
                    @pl.when(short)
                    def _():
                        act(short_copy(j))

    def group_copy(g, j, far):
        begin, count = GROUPS[g]
        begin, count = begin * unit, count * unit
        there = pl.ds(pl.multiple_of(me * rows + begin, unit), count)
        columns = slice(LANES, None) if far else slice(None)
        return remote(
            narrow.at[0, j, begin : begin + count, columns], final_gate.at[0, there, columns],
            group_send.at[g, j], group_recv.at[g, j], peer(j),
        )

    def each_group_copy(g, sending, act):
        @pl.loop(1, members)
        def _(j):
            other = peer(j) if sending else back(j)

            @pl.when(is_far(other))
            def _():
                act(group_copy(g, j, True))

            @pl.when(jnp.logical_not(is_far(other)))
            def _():
                act(group_copy(g, j, False))

    def first_copy(j):
        return remote(first.at[j], first_in.at[j], first_send.at[j], first_recv.at[j], peer(j))

    def first_scale_copy(j):
        return remote(
            first_scales.at[0], first_scales.at[j], fscale_send.at[j], fscale_recv.at[j], peer(j)
        )

    def raw_copy(piece, n):
        count = rows // 2
        part = slice(piece * count, (piece + 1) * count)
        return remote(
            raw.at[n, part, :], stage.at[n, part, :],
            raw_send.at[piece, n], raw_recv.at[piece, n], far_peer(n),
        )

    def near_copy(n, far):
        owner = far_peer(n) if far else near_peer(n)
        return remote(
            late.at[offset(owner)], (far_in if far else near_in).at[n],
            near_send.at[int(far), n], near_recv.at[int(far), n], near_peer(n),
        )

    def cross_copy():
        return remote(total_far, far_total, cross_send.at[0], cross_recv.at[0], far_peer(0))

    def scale_copy(n):
        return remote(scales.at[0], scales.at[n], scale_send.at[n], scale_recv.at[n], near_peer(n))

    def far_scale_copy():
        return remote(
            scales.at[0], scales.at[half], scale_send.at[0], scale_recv.at[0], far_peer(0)
        )

    def relay_scale_copy(n):
        return remote(
            scales.at[half], scales.at[half + n], relay_send.at[n], relay_recv.at[n], near_peer(n)
        )

    def scale_slot(device):
        n = lax.rem(place_in_half + half - lax.rem(device, half), half)
        return jnp.where(is_far(device), half, 0) + n

    width, depth = part_router.shape
    my_group_rows = pl.ds(pl.multiple_of(group * width, width), width)
    my_columns = pl.ds(pl.multiple_of(me * depth, depth), depth)
    near = [*range(1, half), half]

    def row_peer(j):
        return far_peer(0) if j == half else near_peer(j)

    def row_copy(j):
        return remote(
            part_router, router.at[my_group_rows, my_columns],
            row_send.at[j], row_recv.at[j], row_peer(j),
        )

    def relay_copy(j):
        other = pl.ds(pl.multiple_of(far_peer(0) * depth, depth), depth)
        block = router.at[my_group_rows, other]
        return remote(block, block, row_send.at[half + j], row_recv.at[half + j], near_peer(j))

    def col_copy(j):
        return pltpu.make_async_remote_copy(
            src_ref=router.at[my_group_rows, :], dst_ref=router.at[my_group_rows, :],
            send_sem=col_send.at[j], recv_sem=col_recv.at[j],
            device_id=(group_peer(j), me), device_id_type=MESH,
        )

    barrier = pltpu.get_barrier_semaphore()
    for j in range(1, members):
        pl.semaphore_signal(barrier, inc=1, device_id=(group, peer(j)), device_id_type=MESH)
    for j in range(1, groups):
        pl.semaphore_signal(barrier, inc=1, device_id=(group_peer(j), me), device_id_type=MESH)

    start_load(0, 0)
    for place in range(RING):
        start_place(place)
    weight_copy = pltpu.make_async_copy(weight, weight_in, in_sem.at[0])
    gain_copy = pltpu.make_async_copy(gain, gain_in, in_sem.at[1])
    weight_copy.start()
    gain_copy.start()

    def sums(step, slot):
        @pl.loop(0, members)
        def _(j):
            load(step, slot, j).wait()
            block = held[slot, j]
            value = jnp.sum(block * block, axis=0, keepdims=True)
            if step == 0:
                first[j] = value
            else:
                late[j, step - 1] = value

    def late_sums(begin, end):
        for step in range(begin, min(end, steps)):
            sums(step, 1 + (step - 1) % RING)
            start_place(step - 1 + RING)

    def finish(step, value):
        index = step % local
        (scale_gate, scale_up)[step // local][index : index + 1, :] = value

    def keep_own(step, slot, inverse):
        _, final, index = source(step)
        final[index, rows_of(me), :] = (held[slot, 0] * inverse).astype(jnp.bfloat16)

    sums(0, 0)

    pl.semaphore_wait(barrier, members + groups - 2)

    @pl.loop(1, members)
    def _(j):
        first_copy(j).start()

    @pl.loop(0, half)
    def _(n):
        raw[n] = held[0, offset(far_peer(n)), :, 0:LANES].astype(jnp.bfloat16)

    @pl.loop(0, half)
    def _(n):
        raw_copy(0, n).start()

    late_sums(1, 3)

    @pl.loop(1, members)
    def _(j):
        first_copy(j).wait_recv()

    value = first[0]
    for j in range(1, members):
        value = value + first_in[j]
    value = jnp.sqrt(value)
    first_scales[0] = value
    finish(0, value)

    @pl.loop(1, members)
    def _(j):
        first_scale_copy(j).start()

    @pl.loop(0, half)
    def _(n):
        raw_copy(1, n).start()

    late_sums(3, 6)

    @pl.loop(1, members)
    def _(j):
        first_scale_copy(j).wait_recv()

    @pl.loop(1, members)
    def _(j):
        inverse = 1.0 / first_scales[lax.rem(members - j, members)]
        narrow[0, j] = (held[0, j] * inverse).astype(jnp.bfloat16)

    def start_group(g):
        each_group_copy(g, True, lambda copy: copy.start())

    start_group(0)

    late_sums(6, steps)

    for n in range(1, half):
        for far in (True, False):
            near_copy(n, far).start()

    start_group(1)

    my_inverse = 1.0 / first_scales[0]
    keep_own(0, 0, my_inverse)

    weight_copy.wait()
    gain_copy.wait()
    part_router[...] = (weight_in[...] * gain_in[...]).astype(jnp.bfloat16)
    router[my_group_rows, my_columns] = part_router[...]

    @pl.loop(0, half)
    def _(n):
        for piece in range(2):
            raw_copy(piece, n).wait_recv()
        from_member = (1 - side) * half + lax.rem(place_in_half + half - n, half)
        block = stage[n].astype(jnp.float32) * my_inverse[:, 0:LANES]
        final_gate[0, rows_of(from_member), 0:LANES] = block.astype(jnp.bfloat16)

    for n in range(1, half):
        for far in (True, False):
            near_copy(n, far).wait_recv()
    gathered = late[half]
    for n in range(1, half):
        gathered = gathered + far_in[n]
    total_far[...] = gathered
    cross_copy().start()

    start_group(2)

    gathered = late[0]
    for n in range(1, half):
        gathered = gathered + near_in[n]
    cross_copy().wait_recv()
    scales[0] = jnp.sqrt(gathered + far_total[...])
    far_scale_copy().start()
    for n in range(1, half):
        scale_copy(n).start()

    start_group(3)

    for step in range(1, steps):
        finish(step, scales[0, step - 1])

    far_scale_copy().wait_recv()
    for n in range(1, half):
        relay_scale_copy(n).start()

    start_group(4)

    for j in near:
        row_copy(j).start()

    for n in range(1, half):
        scale_copy(n).wait_recv()
        relay_scale_copy(n).wait_recv()

    def wait_sent(step):
        if step == 0:
            for g in range(len(GROUPS)):
                each_group_copy(g, True, lambda copy: copy.wait_send())
        else:
            each_data_copy(step, True, lambda copy: copy.wait_send())

    def scale_and_send(step, slot):
        if step >= SLOTS:
            wait_sent(step - SLOTS)

        @pl.loop(1, members)
        def _(j):
            load(step, slot, j).wait()
            inverse = 1.0 / scales[scale_slot(peer(j)), step - 1]
            narrow[step % SLOTS, j] = (held[slot, j] * inverse).astype(jnp.bfloat16)

        each_data_copy(step, True, lambda copy: copy.start())
        if step == steps - 1:
            kept[...] = narrow[step % SLOTS, offset(partner), rows - kept_rows :]

        load(step, slot, 0).wait()
        keep_own(step, slot, 1.0 / scales[0, step - 1])

    for step in range(1, steps):
        place = steps - 2 + step
        scale_and_send(step, 1 + place % RING)
        start_place(place + RING)
        if step == steps // 2:
            for j in near:
                row_copy(j).wait()
            for j in range(1, half):
                relay_copy(j).start()

    for j in range(1, half):
        relay_copy(j).wait()
    for j in range(1, groups):
        col_copy(j).start()

    @pl.loop(1, members)
    def _(j):
        first_copy(j).wait_send()
        first_scale_copy(j).wait_send()

    @pl.loop(0, half)
    def _(n):
        for piece in range(2):
            raw_copy(piece, n).wait_send()

    for n in range(1, half):
        for far in (True, False):
            near_copy(n, far).wait_send()
        scale_copy(n).wait_send()
        relay_scale_copy(n).wait_send()
    cross_copy().wait_send()
    far_scale_copy().wait_send()

    for j in range(1, groups):
        col_copy(j).wait()

    @pl.loop(0, router.shape[1] // LANES)
    def _(block):
        here = pl.ds(pl.multiple_of(block * LANES, LANES), LANES)
        serve[here, :] = router[:, here].astype(jnp.float32).T.astype(jnp.bfloat16)

    for step in range(steps):
        if step >= steps - SLOTS:
            wait_sent(step)
        if step == 0:
            for g in range(len(GROUPS)):
                each_group_copy(g, False, lambda copy: copy.wait_recv())
        else:
            each_data_copy(step, False, lambda copy: copy.wait_recv())


def exchange(groups, members, master_gate, master_up, weight, gain):
    experts, rows, inner = master_gate.shape
    local = experts // members
    steps = 2 * local
    half = members // 2
    width, depth = weight.shape
    in_hbm = pl.BlockSpec(memory_space=pltpu.HBM)
    in_vmem = pl.BlockSpec(memory_space=pltpu.VMEM)
    final = pltpu.VMEM((local, members * rows, inner), jnp.bfloat16)
    scale = pltpu.VMEM((local, inner), jnp.float32)
    dma = pltpu.SemaphoreType.DMA

    def sums(*shape):
        return pltpu.VMEM((*shape, 1, inner), jnp.float32)

    late = steps - 1
    return pl.pallas_call(
        functools.partial(kernel, groups, members, local, rows),
        out_shape=(
            final, final, scale, scale,
            pltpu.VMEM((members * depth, groups * width), jnp.bfloat16),
            pltpu.VMEM((rows // UNITS * KEPT_UNITS, inner), jnp.bfloat16),
        ),
        in_specs=[in_hbm] * 4,
        out_specs=(in_vmem,) * 6,
        scratch_shapes=[
            pltpu.VMEM((1 + RING, members, rows, inner), jnp.float32),
            pltpu.VMEM((SLOTS, members, rows, inner), jnp.bfloat16),
            pltpu.VMEM((half, rows, LANES), jnp.bfloat16),
            pltpu.VMEM((half, rows, LANES), jnp.bfloat16),
            sums(members), sums(members), sums(members),
            sums(members, late), sums(half, late), sums(half, late),
            sums(late), sums(late), sums(members, late),
            pltpu.VMEM((width, depth), jnp.float32),
            pltpu.VMEM((1, depth), jnp.float32),
            pltpu.VMEM((width, depth), jnp.bfloat16),
            pltpu.VMEM((groups * width, members * depth), jnp.bfloat16),
            dma((1 + RING, members)),
            dma((steps, members)), dma((steps, members)),
            dma((len(GROUPS), members)), dma((len(GROUPS), members)),
            dma((members,)), dma((members,)), dma((members,)), dma((members,)),
            dma((2, half)), dma((2, half)), dma((2, half)), dma((2, half)), dma((1,)), dma((1,)),
            dma((half,)), dma((half,)), dma((half,)), dma((half,)),
            dma((members,)), dma((members,)), dma((groups,)), dma((groups,)), dma((2,)),
        ],
        compiler_params=pltpu.CompilerParams(
            collective_id=0, has_side_effects=True, vmem_limit_bytes=35 * 1024 * 1024
        ),
    )(master_gate, master_up, weight, gain)


def store_kernel(*refs):
    count = (len(refs) - 1) // 2
    sem = refs[-1]
    copies = []
    for landed, stored in zip(refs[:count], refs[count:-1]):
        if len(landed.shape) == 3:
            pairs = [(landed.at[i], stored.at[i]) for i in range(landed.shape[0])]
        else:
            pairs = [(landed, stored)]
        for here, there in pairs:
            copies.append(pltpu.make_async_copy(here, there, sem.at[len(copies)]))
    for copy in copies:
        copy.start()
    for copy in copies:
        copy.wait()


def store(*landed):
    pieces = sum(array.shape[0] if array.ndim == 3 else 1 for array in landed)
    return pl.pallas_call(
        store_kernel,
        out_shape=tuple(jax.ShapeDtypeStruct(array.shape, array.dtype) for array in landed),
        in_specs=[pl.BlockSpec(memory_space=pltpu.VMEM)] * len(landed),
        out_specs=(pl.BlockSpec(memory_space=pl.ANY),) * len(landed),
        cost_estimate=pl.CostEstimate(flops=20_000_000, bytes_accessed=1000, transcendentals=0),
        scratch_shapes=[pltpu.SemaphoreType.DMA((pieces,))],
        compiler_params=pltpu.CompilerParams(vmem_limit_bytes=2 * 1024 * 1024),
    )(*landed)


def place_kernel(members, rows, moved, whole, placed, sem):
    del whole
    me = lax.axis_index("fsdp")
    count = moved.shape[0]

    @pl.when(in_middle(me, members))
    def _():
        begin = partner_of(me, members) * rows + (rows - count)
        there = pl.ds(pl.multiple_of(begin, rows // UNITS), count)
        copy = pltpu.make_async_copy(moved, placed.at[placed.shape[0] - 1, there, :], sem.at[0])
        copy.start()
        copy.wait()


def place(members, rows, moved, whole):
    anywhere = pl.BlockSpec(memory_space=pl.ANY)
    return pl.pallas_call(
        functools.partial(place_kernel, members, rows),
        out_shape=jax.ShapeDtypeStruct(whole.shape, whole.dtype),
        in_specs=[pl.BlockSpec(memory_space=pltpu.VMEM), anywhere],
        out_specs=anywhere,
        input_output_aliases={1: 0},
        scratch_shapes=[pltpu.SemaphoreType.DMA((1,))],
        compiler_params=pltpu.CompilerParams(vmem_limit_bytes=2 * 1024 * 1024),
    )(moved, whole)


def solution(mesh):
    groups, members = mesh.shape["ep"], mesh.shape["fsdp"]

    def body(master_gate, master_up, router_weight, router_gain):
        *landed, kept = exchange(
            groups, members, master_gate, master_up, router_weight.T, router_gain[None, :]
        )
        low = range(members // 4, members // 2)
        pairs = [(i, i + members // 4) for i in low] + [(i + members // 4, i) for i in low]
        moved = lax.ppermute(kept, "fsdp", pairs)
        final_gate, final_up, *rest = store(*landed)
        final_up = place(members, master_gate.shape[1], moved, final_up)
        return (final_gate, final_up, *rest)

    return jax.shard_map(
        body,
        mesh=mesh,
        in_specs=(P("ep", "fsdp", None), P("ep", "fsdp", None), P("fsdp", "ep"), P("fsdp")),
        out_specs=(
            P(("ep", "fsdp"), None, None),
            P(("ep", "fsdp"), None, None),
            P(("ep", "fsdp"), None),
            P(("ep", "fsdp"), None),
            P(),
        ),
        check_vma=False,
    )
```

```python
import functools

import jax
import jax.numpy as jnp
from jax import lax
from jax.experimental import pallas as pl
from jax.experimental.pallas import tpu as pltpu
from jax.sharding import PartitionSpec as P

MESH = pl.DeviceIdType.MESH
RING = 2
SLOTS = 3
LANES = 128
UNITS = 8
GROUPS = ((0, 1), (1, 2), (3, 2), (5, 1), (6, 2))
KEPT_UNITS = (8, 8, 4)


def takes_part(group, member, members):
    middle = jnp.logical_and(member >= members // 4, member < members - members // 4)
    return jnp.logical_and(middle, lax.rem(group, 2) == 1)


def kept_rows_of(local, rows):
    unit = rows // UNITS
    return {2 * local - 1 - i: count * unit for i, count in enumerate(KEPT_UNITS[:local])}


def partner_of(member, members):
    return jnp.where(member < members // 2, member + members // 4, member - members // 4)


def kernel(
    groups, members, local, rows,
    gate, up, weight, gain,
    final_gate, final_up, scale_gate, scale_up, serve, kept,
    held, narrow, raw, stage,
    first, first_in, first_scales,
    late, near_in, far_in, total_far, far_total, scales,
    weight_in, gain_in, part_router, router,
    load_sem, send_sem, recv_sem, group_send, group_recv,
    first_send, first_recv, fscale_send, fscale_recv,
    raw_send, raw_recv, near_send, near_recv, cross_send, cross_recv,
    scale_send, scale_recv, relay_send, relay_recv,
    row_send, row_recv, col_send, col_recv, in_sem,
):
    group, me = lax.axis_index("ep"), lax.axis_index("fsdp")
    steps = 2 * local
    half = members // 2
    side, place_in_half = me // half, lax.rem(me, half)
    unit = rows // UNITS

    def peer(j):
        return lax.rem(me + j, members)

    def back(j):
        return lax.rem(me + members - j, members)

    def near_peer(n):
        return side * half + lax.rem(place_in_half + n, half)

    def far_peer(n):
        return (1 - side) * half + lax.rem(place_in_half + n, half)

    def offset(device):
        return lax.rem(device + members - me, members)

    def is_far(device):
        return device // half != side

    def group_peer(j):
        return lax.rem(group + j, groups)

    def remote(source, target, send, recv, member):
        return pltpu.make_async_remote_copy(
            src_ref=source, dst_ref=target, send_sem=send, recv_sem=recv,
            device_id=(group, member), device_id_type=MESH,
        )

    def source(step):
        return (gate, up)[step // local], (final_gate, final_up)[step // local], step % local

    order = [*range(1, steps), *range(1, steps)]

    def load(step, slot, j):
        master, _, index = source(step)
        return pltpu.make_async_copy(
            master.at[peer(j) * local + index], held.at[slot, j], load_sem.at[slot, j]
        )

    def start_load(step, slot):
        @pl.loop(0, members)
        def _(j):
            load(step, slot, j).start()

    def start_place(place):
        if place < len(order):
            start_load(order[place], 1 + place % RING)

    def rows_of(member):
        return pl.ds(pl.multiple_of(member * rows, rows), rows)

    def data_copy(step, j):
        _, final, index = source(step)
        return remote(
            narrow.at[step % SLOTS, j], final.at[index, rows_of(me), :],
            send_sem.at[step, j], recv_sem.at[step, j], peer(j),
        )

    kept_rows = kept_rows_of(local, rows)
    partner = partner_of(me, members)

    def short_copy(step, j):
        count = rows - kept_rows[step]
        _, final, index = source(step)
        there = pl.ds(pl.multiple_of(me * rows, rows), count)
        return remote(
            narrow.at[step % SLOTS, j, 0:count], final.at[index, there, :],
            send_sem.at[step, j], recv_sem.at[step, j], peer(j),
        )

    def each_data_copy(step, sending, act):
        @pl.loop(1, members)
        def _(j):
            if step not in kept_rows:
                act(data_copy(step, j))
            else:
                other = peer(j) if sending else back(j)
                short = jnp.logical_and(takes_part(group, me, members), other == partner)

                @pl.when(jnp.logical_not(short))
                def _():
                    act(data_copy(step, j))

                if kept_rows[step] < rows:
                    @pl.when(short)
                    def _():
                        act(short_copy(step, j))

    def group_copy(g, j, far):
        begin, count = GROUPS[g]
        begin, count = begin * unit, count * unit
        there = pl.ds(pl.multiple_of(me * rows + begin, unit), count)
        columns = slice(LANES, None) if far else slice(None)
        return remote(
            narrow.at[0, j, begin : begin + count, columns], final_gate.at[0, there, columns],
            group_send.at[g, j], group_recv.at[g, j], peer(j),
        )

    def each_group_copy(g, sending, act):
        @pl.loop(1, members)
        def _(j):
            other = peer(j) if sending else back(j)

            @pl.when(is_far(other))
            def _():
                act(group_copy(g, j, True))

            @pl.when(jnp.logical_not(is_far(other)))
            def _():
                act(group_copy(g, j, False))

    def first_copy(j):
        return remote(first.at[j], first_in.at[j], first_send.at[j], first_recv.at[j], peer(j))

    def first_scale_copy(j):
        return remote(
            first_scales.at[0], first_scales.at[j], fscale_send.at[j], fscale_recv.at[j], peer(j)
        )

    def raw_copy(piece, n):
        count = rows // 2
        part = slice(piece * count, (piece + 1) * count)
        return remote(
            raw.at[n, part, :], stage.at[n, part, :],
            raw_send.at[piece, n], raw_recv.at[piece, n], far_peer(n),
        )

    def near_copy(n, far):
        owner = far_peer(n) if far else near_peer(n)
        return remote(
            late.at[offset(owner)], (far_in if far else near_in).at[n],
            near_send.at[int(far), n], near_recv.at[int(far), n], near_peer(n),
        )

    def cross_copy():
        return remote(total_far, far_total, cross_send.at[0], cross_recv.at[0], far_peer(0))

    def scale_copy(n):
        return remote(scales.at[0], scales.at[n], scale_send.at[n], scale_recv.at[n], near_peer(n))

    def far_scale_copy():
        return remote(
            scales.at[0], scales.at[half], scale_send.at[0], scale_recv.at[0], far_peer(0)
        )

    def relay_scale_copy(n):
        return remote(
            scales.at[half], scales.at[half + n], relay_send.at[n], relay_recv.at[n], near_peer(n)
        )

    def scale_slot(device):
        n = lax.rem(place_in_half + half - lax.rem(device, half), half)
        return jnp.where(is_far(device), half, 0) + n

    width, depth = part_router.shape
    my_group_rows = pl.ds(pl.multiple_of(group * width, width), width)
    my_columns = pl.ds(pl.multiple_of(me * depth, depth), depth)
    near = [*range(1, half), half]

    def row_peer(j):
        return far_peer(0) if j == half else near_peer(j)

    def row_copy(j):
        return remote(
            part_router, router.at[my_group_rows, my_columns],
            row_send.at[j], row_recv.at[j], row_peer(j),
        )

    def relay_copy(j):
        other = pl.ds(pl.multiple_of(far_peer(0) * depth, depth), depth)
        block = router.at[my_group_rows, other]
        return remote(block, block, row_send.at[half + j], row_recv.at[half + j], near_peer(j))

    def col_copy(j):
        return pltpu.make_async_remote_copy(
            src_ref=router.at[my_group_rows, :], dst_ref=router.at[my_group_rows, :],
            send_sem=col_send.at[j], recv_sem=col_recv.at[j],
            device_id=(group_peer(j), me), device_id_type=MESH,
        )

    barrier = pltpu.get_barrier_semaphore()
    for j in range(1, members):
        pl.semaphore_signal(barrier, inc=1, device_id=(group, peer(j)), device_id_type=MESH)
    for j in range(1, groups):
        pl.semaphore_signal(barrier, inc=1, device_id=(group_peer(j), me), device_id_type=MESH)

    start_load(0, 0)
    for place in range(RING):
        start_place(place)
    weight_copy = pltpu.make_async_copy(weight, weight_in, in_sem.at[0])
    gain_copy = pltpu.make_async_copy(gain, gain_in, in_sem.at[1])
    weight_copy.start()
    gain_copy.start()

    def sums(step, slot):
        @pl.loop(0, members)
        def _(j):
            load(step, slot, j).wait()
            block = held[slot, j]
            value = jnp.sum(block * block, axis=0, keepdims=True)
            if step == 0:
                first[j] = value
            else:
                late[j, step - 1] = value

    def late_sums(begin, end):
        for step in range(begin, min(end, steps)):
            sums(step, 1 + (step - 1) % RING)
            start_place(step - 1 + RING)

    def finish(step, value):
        index = step % local
        (scale_gate, scale_up)[step // local][index : index + 1, :] = value

    def keep_own(step, slot, inverse):
        _, final, index = source(step)
        final[index, rows_of(me), :] = (held[slot, 0] * inverse).astype(jnp.bfloat16)

    sums(0, 0)

    pl.semaphore_wait(barrier, members + groups - 2)

    @pl.loop(1, members)
    def _(j):
        first_copy(j).start()

    @pl.loop(0, half)
    def _(n):
        raw[n] = held[0, offset(far_peer(n)), :, 0:LANES].astype(jnp.bfloat16)

    @pl.loop(0, half)
    def _(n):
        raw_copy(0, n).start()

    late_sums(1, 3)

    @pl.loop(1, members)
    def _(j):
        first_copy(j).wait_recv()

    value = first[0]
    for j in range(1, members):
        value = value + first_in[j]
    value = jnp.sqrt(value)
    first_scales[0] = value
    finish(0, value)

    @pl.loop(1, members)
    def _(j):
        first_scale_copy(j).start()

    @pl.loop(0, half)
    def _(n):
        raw_copy(1, n).start()

    late_sums(3, 6)

    @pl.loop(1, members)
    def _(j):
        first_scale_copy(j).wait_recv()

    @pl.loop(1, members)
    def _(j):
        inverse = 1.0 / first_scales[lax.rem(members - j, members)]
        narrow[0, j] = (held[0, j] * inverse).astype(jnp.bfloat16)

    def start_group(g):
        each_group_copy(g, True, lambda copy: copy.start())

    start_group(0)

    late_sums(6, steps)

    for n in range(1, half):
        for far in (True, False):
            near_copy(n, far).start()

    start_group(1)

    my_inverse = 1.0 / first_scales[0]
    keep_own(0, 0, my_inverse)

    weight_copy.wait()
    gain_copy.wait()
    part_router[...] = (weight_in[...] * gain_in[...]).astype(jnp.bfloat16)
    router[my_group_rows, my_columns] = part_router[...]

    @pl.loop(0, half)
    def _(n):
        for piece in range(2):
            raw_copy(piece, n).wait_recv()
        from_member = (1 - side) * half + lax.rem(place_in_half + half - n, half)
        block = stage[n].astype(jnp.float32) * my_inverse[:, 0:LANES]
        final_gate[0, rows_of(from_member), 0:LANES] = block.astype(jnp.bfloat16)

    for n in range(1, half):
        for far in (True, False):
            near_copy(n, far).wait_recv()
    gathered = late[half]
    for n in range(1, half):
        gathered = gathered + far_in[n]
    total_far[...] = gathered
    cross_copy().start()

    start_group(2)

    gathered = late[0]
    for n in range(1, half):
        gathered = gathered + near_in[n]
    cross_copy().wait_recv()
    scales[0] = jnp.sqrt(gathered + far_total[...])
    far_scale_copy().start()
    for n in range(1, half):
        scale_copy(n).start()

    start_group(3)

    for step in range(1, steps):
        finish(step, scales[0, step - 1])

    far_scale_copy().wait_recv()
    for n in range(1, half):
        relay_scale_copy(n).start()

    start_group(4)

    for j in near:
        row_copy(j).start()

    for n in range(1, half):
        scale_copy(n).wait_recv()
        relay_scale_copy(n).wait_recv()

    def wait_sent(step):
        if step == 0:
            for g in range(len(GROUPS)):
                each_group_copy(g, True, lambda copy: copy.wait_send())
        else:
            each_data_copy(step, True, lambda copy: copy.wait_send())

    def scale_and_send(step, slot):
        if step >= SLOTS:
            wait_sent(step - SLOTS)

        @pl.loop(1, members)
        def _(j):
            load(step, slot, j).wait()
            inverse = 1.0 / scales[scale_slot(peer(j)), step - 1]
            narrow[step % SLOTS, j] = (held[slot, j] * inverse).astype(jnp.bfloat16)

        each_data_copy(step, True, lambda copy: copy.start())
        if step in kept_rows:
            count = kept_rows[step]
            begin = sum(size for other, size in kept_rows.items() if other > step)
            kept[begin : begin + count] = narrow[step % SLOTS, offset(partner), rows - count :]

        load(step, slot, 0).wait()
        keep_own(step, slot, 1.0 / scales[0, step - 1])

    for step in range(1, steps):
        place = steps - 2 + step
        scale_and_send(step, 1 + place % RING)
        start_place(place + RING)
        if step == steps // 2:
            for j in near:
                row_copy(j).wait()
            for j in range(1, half):
                relay_copy(j).start()

    for j in range(1, half):
        relay_copy(j).wait()
    for j in range(1, groups):
        col_copy(j).start()

    @pl.loop(1, members)
    def _(j):
        first_copy(j).wait_send()
        first_scale_copy(j).wait_send()

    @pl.loop(0, half)
    def _(n):
        for piece in range(2):
            raw_copy(piece, n).wait_send()

    for n in range(1, half):
        for far in (True, False):
            near_copy(n, far).wait_send()
        scale_copy(n).wait_send()
        relay_scale_copy(n).wait_send()
    cross_copy().wait_send()
    far_scale_copy().wait_send()

    for j in range(1, groups):
        col_copy(j).wait()

    @pl.loop(0, router.shape[1] // LANES)
    def _(block):
        here = pl.ds(pl.multiple_of(block * LANES, LANES), LANES)
        serve[here, :] = router[:, here].astype(jnp.float32).T.astype(jnp.bfloat16)

    for step in range(steps):
        if step >= steps - SLOTS:
            wait_sent(step)
        if step == 0:
            for g in range(len(GROUPS)):
                each_group_copy(g, False, lambda copy: copy.wait_recv())
        else:
            each_data_copy(step, False, lambda copy: copy.wait_recv())


def exchange(groups, members, master_gate, master_up, weight, gain):
    experts, rows, inner = master_gate.shape
    local = experts // members
    steps = 2 * local
    half = members // 2
    width, depth = weight.shape
    in_hbm = pl.BlockSpec(memory_space=pltpu.HBM)
    in_vmem = pl.BlockSpec(memory_space=pltpu.VMEM)
    final = pltpu.VMEM((local, members * rows, inner), jnp.bfloat16)
    scale = pltpu.VMEM((local, inner), jnp.float32)
    dma = pltpu.SemaphoreType.DMA

    def sums(*shape):
        return pltpu.VMEM((*shape, 1, inner), jnp.float32)

    late = steps - 1
    return pl.pallas_call(
        functools.partial(kernel, groups, members, local, rows),
        out_shape=(
            final, final, scale, scale,
            pltpu.VMEM((members * depth, groups * width), jnp.bfloat16),
            pltpu.VMEM((sum(kept_rows_of(local, rows).values()), inner), jnp.bfloat16),
        ),
        in_specs=[in_hbm] * 4,
        out_specs=(in_vmem,) * 6,
        scratch_shapes=[
            pltpu.VMEM((1 + RING, members, rows, inner), jnp.float32),
            pltpu.VMEM((SLOTS, members, rows, inner), jnp.bfloat16),
            pltpu.VMEM((half, rows, LANES), jnp.bfloat16),
            pltpu.VMEM((half, rows, LANES), jnp.bfloat16),
            sums(members), sums(members), sums(members),
            sums(members, late), sums(half, late), sums(half, late),
            sums(late), sums(late), sums(members, late),
            pltpu.VMEM((width, depth), jnp.float32),
            pltpu.VMEM((1, depth), jnp.float32),
            pltpu.VMEM((width, depth), jnp.bfloat16),
            pltpu.VMEM((groups * width, members * depth), jnp.bfloat16),
            dma((1 + RING, members)),
            dma((steps, members)), dma((steps, members)),
            dma((len(GROUPS), members)), dma((len(GROUPS), members)),
            dma((members,)), dma((members,)), dma((members,)), dma((members,)),
            dma((2, half)), dma((2, half)), dma((2, half)), dma((2, half)), dma((1,)), dma((1,)),
            dma((half,)), dma((half,)), dma((half,)), dma((half,)),
            dma((members,)), dma((members,)), dma((groups,)), dma((groups,)), dma((2,)),
        ],
        compiler_params=pltpu.CompilerParams(
            collective_id=0, has_side_effects=True, vmem_limit_bytes=35 * 1024 * 1024
        ),
    )(master_gate, master_up, weight, gain)


def store_kernel(*refs):
    count = (len(refs) - 1) // 2
    sem = refs[-1]
    copies = []
    for landed, stored in zip(refs[:count], refs[count:-1]):
        if len(landed.shape) == 3:
            pairs = [(landed.at[i], stored.at[i]) for i in range(landed.shape[0])]
        else:
            pairs = [(landed, stored)]
        for here, there in pairs:
            copies.append(pltpu.make_async_copy(here, there, sem.at[len(copies)]))
    for copy in copies:
        copy.start()
    for copy in copies:
        copy.wait()


def store(*landed):
    pieces = sum(array.shape[0] if array.ndim == 3 else 1 for array in landed)
    return pl.pallas_call(
        store_kernel,
        out_shape=tuple(jax.ShapeDtypeStruct(array.shape, array.dtype) for array in landed),
        in_specs=[pl.BlockSpec(memory_space=pltpu.VMEM)] * len(landed),
        out_specs=(pl.BlockSpec(memory_space=pl.ANY),) * len(landed),
        cost_estimate=pl.CostEstimate(flops=20_000_000, bytes_accessed=1000, transcendentals=0),
        scratch_shapes=[pltpu.SemaphoreType.DMA((pieces,))],
        compiler_params=pltpu.CompilerParams(vmem_limit_bytes=2 * 1024 * 1024),
    )(*landed)


def place_kernel(members, rows, moved, whole, placed, sem):
    del whole
    group, me = lax.axis_index("ep"), lax.axis_index("fsdp")
    local = placed.shape[0]

    @pl.when(takes_part(group, me, members))
    def _():
        copies, begin = [], 0
        for step, count in kept_rows_of(local, rows).items():
            first = partner_of(me, members) * rows + (rows - count)
            there = pl.ds(pl.multiple_of(first, rows // UNITS), count)
            copies.append(
                pltpu.make_async_copy(
                    moved.at[begin : begin + count], placed.at[step - local, there, :],
                    sem.at[len(copies)],
                )
            )
            begin += count
        for copy in copies:
            copy.start()
        for copy in copies:
            copy.wait()


def place(members, rows, moved, whole):
    anywhere = pl.BlockSpec(memory_space=pl.ANY)
    return pl.pallas_call(
        functools.partial(place_kernel, members, rows),
        out_shape=jax.ShapeDtypeStruct(whole.shape, whole.dtype),
        in_specs=[pl.BlockSpec(memory_space=pltpu.VMEM), anywhere],
        out_specs=anywhere,
        input_output_aliases={1: 0},
        scratch_shapes=[pltpu.SemaphoreType.DMA((len(KEPT_UNITS),))],
        compiler_params=pltpu.CompilerParams(vmem_limit_bytes=2 * 1024 * 1024),
    )(moved, whole)


def solution(mesh):
    groups, members = mesh.shape["ep"], mesh.shape["fsdp"]

    def body(master_gate, master_up, router_weight, router_gain):
        *landed, kept = exchange(
            groups, members, master_gate, master_up, router_weight.T, router_gain[None, :]
        )
        low = [
            g * members + i
            for g in range(1, groups, 2)
            for i in range(members // 4, members // 2)
        ]
        pairs = [(i, i + members // 4) for i in low] + [(i + members // 4, i) for i in low]
        moved = lax.ppermute(kept, ("ep", "fsdp"), pairs)
        final_gate, final_up, *rest = store(*landed)
        final_up = place(members, master_gate.shape[1], moved, final_up)
        return (final_gate, final_up, *rest)

    return jax.shard_map(
        body,
        mesh=mesh,
        in_specs=(P("ep", "fsdp", None), P("ep", "fsdp", None), P("fsdp", "ep"), P("fsdp")),
        out_specs=(
            P(("ep", "fsdp"), None, None),
            P(("ep", "fsdp"), None, None),
            P(("ep", "fsdp"), None),
            P(("ep", "fsdp"), None),
            P(),
        ),
        check_vma=False,
    )
```

```python
import functools

import jax
import jax.numpy as jnp
from jax import lax
from jax.experimental import pallas as pl
from jax.experimental.pallas import tpu as pltpu
from jax.sharding import PartitionSpec as P

MESH = pl.DeviceIdType.MESH
RING = 2
SLOTS = 3
LANES = 128
EARLY_UNITS = 3
UNITS = 8
GROUPS = ((0, 1), (1, 2), (3, 2), (5, 1), (6, 2))
KEPT_UNITS = (8, 8, 4)


def takes_part(group, member, members):
    middle = jnp.logical_and(member >= members // 4, member < members - members // 4)
    return jnp.logical_and(middle, lax.rem(group, 2) == 1)


def kept_rows_of(local, rows):
    unit = rows // UNITS
    return {2 * local - 1 - i: count * unit for i, count in enumerate(KEPT_UNITS[:local])}


def partner_of(member, members):
    return jnp.where(member < members // 2, member + members // 4, member - members // 4)


def kernel(
    groups, members, local, rows,
    gate, up, weight, gain,
    final_gate, final_up, scale_gate, scale_up, serve, kept,
    held, narrow, raw, stage,
    first, first_in, first_scales,
    late, near_in, far_in, total_far, far_total, scales,
    weight_in, gain_in, part_router, router,
    load_sem, send_sem, recv_sem, group_send, group_recv,
    first_send, first_recv, fscale_send, fscale_recv,
    raw_send, raw_recv, near_send, near_recv, cross_send, cross_recv,
    scale_send, scale_recv, relay_send, relay_recv,
    row_send, row_recv, col_send, col_recv, in_sem,
):
    group, me = lax.axis_index("ep"), lax.axis_index("fsdp")
    steps = 2 * local
    half = members // 2
    side, place_in_half = me // half, lax.rem(me, half)
    unit = rows // UNITS
    early = EARLY_UNITS * unit

    def peer(j):
        return lax.rem(me + j, members)

    def back(j):
        return lax.rem(me + members - j, members)

    def near_peer(n):
        return side * half + lax.rem(place_in_half + n, half)

    def far_peer(n):
        return (1 - side) * half + lax.rem(place_in_half + n, half)

    def offset(device):
        return lax.rem(device + members - me, members)

    def is_far(device):
        return device // half != side

    def group_peer(j):
        return lax.rem(group + j, groups)

    def remote(source, target, send, recv, member):
        return pltpu.make_async_remote_copy(
            src_ref=source, dst_ref=target, send_sem=send, recv_sem=recv,
            device_id=(group, member), device_id_type=MESH,
        )

    def source(step):
        return (gate, up)[step // local], (final_gate, final_up)[step // local], step % local

    order = [*range(1, steps), *range(1, steps)]

    def load(step, slot, j):
        master, _, index = source(step)
        return pltpu.make_async_copy(
            master.at[peer(j) * local + index], held.at[slot, j], load_sem.at[slot, j]
        )

    def start_load(step, slot):
        @pl.loop(0, members)
        def _(j):
            load(step, slot, j).start()

    def start_place(place):
        if place < len(order):
            start_load(order[place], 1 + place % RING)

    def rows_of(member):
        return pl.ds(pl.multiple_of(member * rows, rows), rows)

    def data_copy(step, j):
        _, final, index = source(step)
        return remote(
            narrow.at[step % SLOTS, j], final.at[index, rows_of(me), :],
            send_sem.at[step, j], recv_sem.at[step, j], peer(j),
        )

    kept_rows = kept_rows_of(local, rows)
    partner = partner_of(me, members)

    def short_copy(step, j):
        count = rows - kept_rows[step]
        _, final, index = source(step)
        there = pl.ds(pl.multiple_of(me * rows, rows), count)
        return remote(
            narrow.at[step % SLOTS, j, 0:count], final.at[index, there, :],
            send_sem.at[step, j], recv_sem.at[step, j], peer(j),
        )

    def each_data_copy(step, sending, act):
        @pl.loop(1, members)
        def _(j):
            if step not in kept_rows:
                act(data_copy(step, j))
            else:
                other = peer(j) if sending else back(j)
                short = jnp.logical_and(takes_part(group, me, members), other == partner)

                @pl.when(jnp.logical_not(short))
                def _():
                    act(data_copy(step, j))

                if kept_rows[step] < rows:
                    @pl.when(short)
                    def _():
                        act(short_copy(step, j))

    def group_copy(g, j, far):
        begin, count = GROUPS[g]
        begin, count = begin * unit, count * unit
        there = pl.ds(pl.multiple_of(me * rows + begin, unit), count)
        columns = slice(LANES, None) if far and begin < early else slice(None)
        return remote(
            narrow.at[0, j, begin : begin + count, columns], final_gate.at[0, there, columns],
            group_send.at[g, j], group_recv.at[g, j], peer(j),
        )

    def each_group_copy(g, sending, act):
        @pl.loop(1, members)
        def _(j):
            other = peer(j) if sending else back(j)

            @pl.when(is_far(other))
            def _():
                act(group_copy(g, j, True))

            @pl.when(jnp.logical_not(is_far(other)))
            def _():
                act(group_copy(g, j, False))

    def first_copy(j):
        return remote(first.at[j], first_in.at[j], first_send.at[j], first_recv.at[j], peer(j))

    def first_scale_copy(j):
        return remote(
            first_scales.at[0], first_scales.at[j], fscale_send.at[j], fscale_recv.at[j], peer(j)
        )

    def raw_copy(piece, n):
        count = early // 2
        part = slice(piece * count, (piece + 1) * count)
        return remote(
            raw.at[n, part, :], stage.at[n, part, :],
            raw_send.at[piece, n], raw_recv.at[piece, n], far_peer(n),
        )

    def near_copy(n, far):
        owner = far_peer(n) if far else near_peer(n)
        return remote(
            late.at[offset(owner)], (far_in if far else near_in).at[n],
            near_send.at[int(far), n], near_recv.at[int(far), n], near_peer(n),
        )

    def cross_copy():
        return remote(total_far, far_total, cross_send.at[0], cross_recv.at[0], far_peer(0))

    def scale_copy(n):
        return remote(scales.at[0], scales.at[n], scale_send.at[n], scale_recv.at[n], near_peer(n))

    def far_scale_copy():
        return remote(
            scales.at[0], scales.at[half], scale_send.at[0], scale_recv.at[0], far_peer(0)
        )

    def relay_scale_copy(n):
        return remote(
            scales.at[half], scales.at[half + n], relay_send.at[n], relay_recv.at[n], near_peer(n)
        )

    def scale_slot(device):
        n = lax.rem(place_in_half + half - lax.rem(device, half), half)
        return jnp.where(is_far(device), half, 0) + n

    width, depth = part_router.shape
    my_group_rows = pl.ds(pl.multiple_of(group * width, width), width)
    my_columns = pl.ds(pl.multiple_of(me * depth, depth), depth)
    near = [*range(1, half), half]

    def row_peer(j):
        return far_peer(0) if j == half else near_peer(j)

    def row_copy(j):
        return remote(
            part_router, router.at[my_group_rows, my_columns],
            row_send.at[j], row_recv.at[j], row_peer(j),
        )

    def relay_copy(j):
        other = pl.ds(pl.multiple_of(far_peer(0) * depth, depth), depth)
        block = router.at[my_group_rows, other]
        return remote(block, block, row_send.at[half + j], row_recv.at[half + j], near_peer(j))

    def col_copy(j):
        return pltpu.make_async_remote_copy(
            src_ref=router.at[my_group_rows, :], dst_ref=router.at[my_group_rows, :],
            send_sem=col_send.at[j], recv_sem=col_recv.at[j],
            device_id=(group_peer(j), me), device_id_type=MESH,
        )

    barrier = pltpu.get_barrier_semaphore()
    for j in range(1, members):
        pl.semaphore_signal(barrier, inc=1, device_id=(group, peer(j)), device_id_type=MESH)
    for j in range(1, groups):
        pl.semaphore_signal(barrier, inc=1, device_id=(group_peer(j), me), device_id_type=MESH)

    start_load(0, 0)
    for place in range(RING):
        start_place(place)
    weight_copy = pltpu.make_async_copy(weight, weight_in, in_sem.at[0])
    gain_copy = pltpu.make_async_copy(gain, gain_in, in_sem.at[1])
    weight_copy.start()
    gain_copy.start()

    def sums(step, slot):
        @pl.loop(0, members)
        def _(j):
            load(step, slot, j).wait()
            block = held[slot, j]
            value = jnp.sum(block * block, axis=0, keepdims=True)
            if step == 0:
                first[j] = value
            else:
                late[j, step - 1] = value

    def late_sums(begin, end):
        for step in range(begin, min(end, steps)):
            sums(step, 1 + (step - 1) % RING)
            start_place(step - 1 + RING)

    def finish(step, value):
        index = step % local
        (scale_gate, scale_up)[step // local][index : index + 1, :] = value

    def keep_own(step, slot, inverse):
        _, final, index = source(step)
        final[index, rows_of(me), :] = (held[slot, 0] * inverse).astype(jnp.bfloat16)

    sums(0, 0)

    pl.semaphore_wait(barrier, members + groups - 2)

    @pl.loop(1, members)
    def _(j):
        first_copy(j).start()

    @pl.loop(0, half)
    def _(n):
        raw[n] = held[0, offset(far_peer(n)), 0:early, 0:LANES]

    @pl.loop(0, half)
    def _(n):
        raw_copy(0, n).start()

    late_sums(1, 3)

    @pl.loop(1, members)
    def _(j):
        first_copy(j).wait_recv()

    value = first[0]
    for j in range(1, members):
        value = value + first_in[j]
    value = jnp.sqrt(value)
    first_scales[0] = value
    finish(0, value)

    @pl.loop(1, members)
    def _(j):
        first_scale_copy(j).start()

    @pl.loop(0, half)
    def _(n):
        raw_copy(1, n).start()

    late_sums(3, 6)

    @pl.loop(1, members)
    def _(j):
        first_scale_copy(j).wait_recv()

    @pl.loop(1, members)
    def _(j):
        inverse = 1.0 / first_scales[lax.rem(members - j, members)]
        narrow[0, j] = (held[0, j] * inverse).astype(jnp.bfloat16)

    def start_group(g):
        each_group_copy(g, True, lambda copy: copy.start())

    start_group(0)

    late_sums(6, steps)

    for n in range(1, half):
        for far in (True, False):
            near_copy(n, far).start()

    start_group(1)

    my_inverse = 1.0 / first_scales[0]
    keep_own(0, 0, my_inverse)

    weight_copy.wait()
    gain_copy.wait()
    part_router[...] = (weight_in[...] * gain_in[...]).astype(jnp.bfloat16)
    router[my_group_rows, my_columns] = part_router[...]

    @pl.loop(0, half)
    def _(n):
        for piece in range(2):
            raw_copy(piece, n).wait_recv()
        from_member = (1 - side) * half + lax.rem(place_in_half + half - n, half)
        block = stage[n] * my_inverse[:, 0:LANES]
        there = pl.ds(pl.multiple_of(from_member * rows, rows), early)
        final_gate[0, there, 0:LANES] = block.astype(jnp.bfloat16)

    for n in range(1, half):
        for far in (True, False):
            near_copy(n, far).wait_recv()
    gathered = late[half]
    for n in range(1, half):
        gathered = gathered + far_in[n]
    total_far[...] = gathered
    cross_copy().start()

    start_group(2)

    gathered = late[0]
    for n in range(1, half):
        gathered = gathered + near_in[n]
    cross_copy().wait_recv()
    scales[0] = jnp.sqrt(gathered + far_total[...])
    far_scale_copy().start()
    for n in range(1, half):
        scale_copy(n).start()

    start_group(3)

    for step in range(1, steps):
        finish(step, scales[0, step - 1])

    far_scale_copy().wait_recv()
    for n in range(1, half):
        relay_scale_copy(n).start()

    start_group(4)

    for j in near:
        row_copy(j).start()

    for n in range(1, half):
        scale_copy(n).wait_recv()
        relay_scale_copy(n).wait_recv()

    def wait_sent(step):
        if step == 0:
            for g in range(len(GROUPS)):
                each_group_copy(g, True, lambda copy: copy.wait_send())
        else:
            each_data_copy(step, True, lambda copy: copy.wait_send())

    def scale_and_send(step, slot):
        if step >= SLOTS:
            wait_sent(step - SLOTS)

        @pl.loop(1, members)
        def _(j):
            load(step, slot, j).wait()
            inverse = 1.0 / scales[scale_slot(peer(j)), step - 1]
            narrow[step % SLOTS, j] = (held[slot, j] * inverse).astype(jnp.bfloat16)

        each_data_copy(step, True, lambda copy: copy.start())
        if step in kept_rows:
            count = kept_rows[step]
            begin = sum(size for other, size in kept_rows.items() if other > step)
            kept[begin : begin + count] = narrow[step % SLOTS, offset(partner), rows - count :]

        load(step, slot, 0).wait()
        keep_own(step, slot, 1.0 / scales[0, step - 1])

    for step in range(1, steps):
        place = steps - 2 + step
        scale_and_send(step, 1 + place % RING)
        start_place(place + RING)
        if step == steps // 2:
            for j in near:
                row_copy(j).wait()
            for j in range(1, half):
                relay_copy(j).start()

    for j in range(1, half):
        relay_copy(j).wait()
    for j in range(1, groups):
        col_copy(j).start()

    @pl.loop(1, members)
    def _(j):
        first_copy(j).wait_send()
        first_scale_copy(j).wait_send()

    @pl.loop(0, half)
    def _(n):
        for piece in range(2):
            raw_copy(piece, n).wait_send()

    for n in range(1, half):
        for far in (True, False):
            near_copy(n, far).wait_send()
        scale_copy(n).wait_send()
        relay_scale_copy(n).wait_send()
    cross_copy().wait_send()
    far_scale_copy().wait_send()

    for j in range(1, groups):
        col_copy(j).wait()

    @pl.loop(0, router.shape[1] // LANES)
    def _(block):
        here = pl.ds(pl.multiple_of(block * LANES, LANES), LANES)
        serve[here, :] = router[:, here].astype(jnp.float32).T.astype(jnp.bfloat16)

    for step in range(steps):
        if step >= steps - SLOTS:
            wait_sent(step)
        if step == 0:
            for g in range(len(GROUPS)):
                each_group_copy(g, False, lambda copy: copy.wait_recv())
        else:
            each_data_copy(step, False, lambda copy: copy.wait_recv())


def exchange(groups, members, master_gate, master_up, weight, gain):
    experts, rows, inner = master_gate.shape
    local = experts // members
    steps = 2 * local
    half = members // 2
    width, depth = weight.shape
    in_hbm = pl.BlockSpec(memory_space=pltpu.HBM)
    in_vmem = pl.BlockSpec(memory_space=pltpu.VMEM)
    final = pltpu.VMEM((local, members * rows, inner), jnp.bfloat16)
    scale = pltpu.VMEM((local, inner), jnp.float32)
    dma = pltpu.SemaphoreType.DMA

    def sums(*shape):
        return pltpu.VMEM((*shape, 1, inner), jnp.float32)

    late = steps - 1
    return pl.pallas_call(
        functools.partial(kernel, groups, members, local, rows),
        out_shape=(
            final, final, scale, scale,
            pltpu.VMEM((members * depth, groups * width), jnp.bfloat16),
            pltpu.VMEM((sum(kept_rows_of(local, rows).values()), inner), jnp.bfloat16),
        ),
        in_specs=[in_hbm] * 4,
        out_specs=(in_vmem,) * 6,
        scratch_shapes=[
            pltpu.VMEM((1 + RING, members, rows, inner), jnp.float32),
            pltpu.VMEM((SLOTS, members, rows, inner), jnp.bfloat16),
            pltpu.VMEM((half, rows // UNITS * EARLY_UNITS, LANES), jnp.float32),
            pltpu.VMEM((half, rows // UNITS * EARLY_UNITS, LANES), jnp.float32),
            sums(members), sums(members), sums(members),
            sums(members, late), sums(half, late), sums(half, late),
            sums(late), sums(late), sums(members, late),
            pltpu.VMEM((width, depth), jnp.float32),
            pltpu.VMEM((1, depth), jnp.float32),
            pltpu.VMEM((width, depth), jnp.bfloat16),
            pltpu.VMEM((groups * width, members * depth), jnp.bfloat16),
            dma((1 + RING, members)),
            dma((steps, members)), dma((steps, members)),
            dma((len(GROUPS), members)), dma((len(GROUPS), members)),
            dma((members,)), dma((members,)), dma((members,)), dma((members,)),
            dma((2, half)), dma((2, half)), dma((2, half)), dma((2, half)), dma((1,)), dma((1,)),
            dma((half,)), dma((half,)), dma((half,)), dma((half,)),
            dma((members,)), dma((members,)), dma((groups,)), dma((groups,)), dma((2,)),
        ],
        compiler_params=pltpu.CompilerParams(
            collective_id=0, has_side_effects=True, vmem_limit_bytes=35 * 1024 * 1024
        ),
    )(master_gate, master_up, weight, gain)


def store_kernel(*refs):
    count = (len(refs) - 1) // 2
    sem = refs[-1]
    copies = []
    for landed, stored in zip(refs[:count], refs[count:-1]):
        if len(landed.shape) == 3:
            pairs = [(landed.at[i], stored.at[i]) for i in range(landed.shape[0])]
        else:
            pairs = [(landed, stored)]
        for here, there in pairs:
            copies.append(pltpu.make_async_copy(here, there, sem.at[len(copies)]))
    for copy in copies:
        copy.start()
    for copy in copies:
        copy.wait()


def store(*landed):
    pieces = sum(array.shape[0] if array.ndim == 3 else 1 for array in landed)
    return pl.pallas_call(
        store_kernel,
        out_shape=tuple(jax.ShapeDtypeStruct(array.shape, array.dtype) for array in landed),
        in_specs=[pl.BlockSpec(memory_space=pltpu.VMEM)] * len(landed),
        out_specs=(pl.BlockSpec(memory_space=pl.ANY),) * len(landed),
        cost_estimate=pl.CostEstimate(flops=20_000_000, bytes_accessed=1000, transcendentals=0),
        scratch_shapes=[pltpu.SemaphoreType.DMA((pieces,))],
        compiler_params=pltpu.CompilerParams(vmem_limit_bytes=2 * 1024 * 1024),
    )(*landed)


def place_kernel(members, rows, moved, whole, placed, sem):
    del whole
    group, me = lax.axis_index("ep"), lax.axis_index("fsdp")
    local = placed.shape[0]

    @pl.when(takes_part(group, me, members))
    def _():
        copies, begin = [], 0
        for step, count in kept_rows_of(local, rows).items():
            first = partner_of(me, members) * rows + (rows - count)
            there = pl.ds(pl.multiple_of(first, rows // UNITS), count)
            copies.append(
                pltpu.make_async_copy(
                    moved.at[begin : begin + count], placed.at[step - local, there, :],
                    sem.at[len(copies)],
                )
            )
            begin += count
        for copy in copies:
            copy.start()
        for copy in copies:
            copy.wait()


def place(members, rows, moved, whole):
    anywhere = pl.BlockSpec(memory_space=pl.ANY)
    return pl.pallas_call(
        functools.partial(place_kernel, members, rows),
        out_shape=jax.ShapeDtypeStruct(whole.shape, whole.dtype),
        in_specs=[pl.BlockSpec(memory_space=pltpu.VMEM), anywhere],
        out_specs=anywhere,
        input_output_aliases={1: 0},
        scratch_shapes=[pltpu.SemaphoreType.DMA((len(KEPT_UNITS),))],
        compiler_params=pltpu.CompilerParams(vmem_limit_bytes=2 * 1024 * 1024),
    )(moved, whole)


def solution(mesh):
    groups, members = mesh.shape["ep"], mesh.shape["fsdp"]

    def body(master_gate, master_up, router_weight, router_gain):
        *landed, kept = exchange(
            groups, members, master_gate, master_up, router_weight.T, router_gain[None, :]
        )
        low = [
            g * members + i
            for g in range(1, groups, 2)
            for i in range(members // 4, members // 2)
        ]
        pairs = [(i, i + members // 4) for i in low] + [(i + members // 4, i) for i in low]
        moved = lax.ppermute(kept, ("ep", "fsdp"), pairs)
        final_gate, final_up, *rest = store(*landed)
        final_up = place(members, master_gate.shape[1], moved, final_up)
        return (final_gate, final_up, *rest)

    return jax.shard_map(
        body,
        mesh=mesh,
        in_specs=(P("ep", "fsdp", None), P("ep", "fsdp", None), P("fsdp", "ep"), P("fsdp")),
        out_specs=(
            P(("ep", "fsdp"), None, None),
            P(("ep", "fsdp"), None, None),
            P(("ep", "fsdp"), None),
            P(("ep", "fsdp"), None),
            P(),
        ),
        check_vma=False,
    )
```
